512 devices in a mesh: hid: 32 (over y, x_hi, core), ep: 16 (over x_lo, z).
Axes of the slice: x: 4 (x_hi: 2, x_lo: 2; x = x_hi * 2 + x_lo), y: 8, z: 8, core: 2. Of those that a mesh axis runs over, the one named last changes fastest.
Arguments:
- tokens: bfloat16 [8192, 2048], P('ep', 'hid'), may hold values from -6 to 6
- expert_ids: int32 [8192, 6], P('ep'), may hold values from 0 to 63, all different within a row; in each aligned block of 512 rows (0 to 511, 512 to 1023, ...) at most 64 rows name the same one
- gate_weights: float32 [8192, 6], P('ep'), may hold values from 0.1 to 1
- w_gate_up: bfloat16 [16, 5632, 2, 2048], P('ep', 'hid'), may hold values from -0.125 to 0.125
- w_down: bfloat16 [16, 5632, 2048], P('ep', 'hid'), may hold values from -0.3125 to 0.3125
Outputs:
- mixed: bfloat16 [8192, 2048], P('ep', 'hid')
The draws below stay inside these ranges and needn't reach their ends.
Inputs may be any that keep to these rules, and one draw needn't show every extreme that they name: `expert_ids`: the 6 ids of a row differ. Among the 512 rows of one index of ep (aligned blocks of rows), no expert is named by more than 64 rows.
All inputs are finite; a program needn't handle non-finite values.
Results may differ from the reference program's by a relative error of at most 0.0064.
Values may be sent and summed in bfloat16 or wider, within the bound.
No kernel may reach another device: no remote copies, remote signals or barrier semaphores. Data moves between devices by JAX's collectives and lax.ppermute only.
A program may use at most 64 MiB of HBM per device.

```python
import math
import jax
import jax.numpy as jnp
import numpy as np
from jax import lax

D = 2048
FF = 1408
TOPK = 6
EXP_DEV = 4
TOK_EP = 512
EXPERTS = 64
SHARDS = 8
CAP = 64
TOKENS = 8192
N_EP = 16


def raised(entries, key, source, target, blocks, factor):
    def block_of(dim):
        return (jnp.arange(entries.shape[dim]) // (entries.shape[dim] // blocks)).reshape((-1,) + (1,) * (entries.ndim - 1 - dim))

    first = jax.random.permutation(key, blocks)[block_of(target)]
    other_side = (block_of(target) + blocks // 2) % blocks
    return jnp.where((block_of(source) == first) | (block_of(source) == other_side), factor * entries, entries)


def steps_of(key, dims, cuts, smallest, largest):
    factor_of, own = 1.0, jax.random.fold_in(key, 6)
    for axis_at, shards_of in cuts:
        draws = jnp.exp(jax.random.uniform(jax.random.fold_in(own, axis_at), (shards_of,), jnp.float32, smallest / len(cuts), largest / len(cuts)))
        factor_of = factor_of * jnp.repeat(draws, dims[axis_at] // shards_of).reshape([-1 if axis == axis_at else 1 for axis in range(len(dims))])
    return factor_of


def assign_block(key, own, number, rows, count, top, bound, lean):
    order = jax.random.permutation(key, count)
    heavy_load, common = portions_of(count, rows * top, bound, lean, True), portions_of(count, rows * top, bound, lean, False)
    places = jnp.arange(count)

    def named(sizes, offset_by):
        used = int((sizes > 0).sum())
        fixed = max(1, used // 4)
        moved = fixed + (places - fixed + offset_by * (used - fixed)) % max(1, count - fixed)
        return jnp.zeros((count,), jnp.int32).at[order[jnp.where(places < fixed, places, moved)]].set(jnp.asarray(sizes, jnp.int32))

    sizes = jnp.where(number % 4 == 0, named(heavy_load, number // 4), named(common, number - number // 4 - 1))
    mixed = jax.random.permutation(jax.random.fold_in(own, 3), count)
    source_of, receiver = mixed[0:count // 2 * 2:2], mixed[1:count // 2 * 2:2]
    margin = jnp.minimum(sizes[source_of] - 1, bound - sizes[receiver]) // 2
    margin = jnp.where((source_of == order[0]) | (receiver == order[0]) | (sizes[receiver] == 0), 0, jnp.maximum(margin, 0))
    moved = jax.random.randint(jax.random.fold_in(own, 4), (count // 2,), 0, 1 << 20) % (margin + 1)
    sizes = sizes.at[source_of].add(-moved).at[receiver].add(moved)
    labels = jnp.searchsorted(jnp.cumsum(sizes), jnp.arange(rows * top), side="right").astype(jnp.int32)
    table = labels.reshape(top, rows).T
    table = table[jax.random.permutation(jax.random.fold_in(own, 1), rows)]
    offset_by = jax.random.randint(jax.random.fold_in(own, 2), (rows, 1), 0, top)
    return jnp.take_along_axis(table, (jnp.arange(top)[None, :] + offset_by) % top, axis=1)


def portions_of(amount, total, limit, slope, full):
    portions = [(1 << 20) // math.isqrt(standing ** slope) + 1 for standing in range(1, amount + 1)]
    largest = limit if full else min(limit, max(-(-total // amount), total * portions[0] // sum(portions)))
    least = 1 if total - largest >= amount - 1 else 0
    given, surplus = [largest] + [least] * (amount - 1), total - largest - least * (amount - 1)
    while surplus > 0:
        free = [i for i in range(1, amount) if given[i] < largest] or [i for i in range(1, amount) if given[i] < limit]
        pool, left = sum([portions[i] for i in free]), surplus
        for i in free:
            extra = min(limit - given[i], max(1, left * portions[i] // pool), surplus)
            given[i] = given[i] + extra
            surplus = surplus - extra
    return np.array(given)


def bell_draw(key, dims, deviation, bound, shards=(), kind=jnp.bfloat16):
    drawn = deviation * jax.random.normal(key, dims, jnp.float32)
    if shards:
        drawn = drawn * steps_of(key, dims, shards, -0.22, 0.18)
    return jnp.clip(drawn, -bound, bound).astype(kind)


def heavy_noise(key, dims, scale, limit, split, heavy, kind=jnp.bfloat16):
    drawn = scale * jax.random.normal(key, dims, jnp.float32)
    if split:
        drawn = drawn * steps_of(key, dims, split, -0.22, 0.18)
    return jnp.clip(raised(drawn, jax.random.fold_in(key, 3), *heavy), -limit, limit).astype(kind)


def setup_inputs(seed: int = 0) -> dict:
    seeds = jax.random.split(jax.random.key(seed), 6)
    tokens = bell_draw(seeds[0], (TOKENS, D), 1.0, 6.0, ((0, 16), (1, 32)))
    expert_ids_keys = jax.random.split(jax.random.fold_in(seeds[1], 1), TOKENS // TOK_EP)
    expert_ids_turns = jax.random.permutation(jax.random.fold_in(seeds[1], 3), TOKENS // TOK_EP)
    expert_ids = jax.vmap(lambda own, number: assign_block(jax.random.fold_in(seeds[1], 2), own, number, TOK_EP, EXPERTS, TOPK, CAP, 2))(expert_ids_keys, expert_ids_turns).reshape((TOKENS, TOPK))
    gate_weights = jnp.clip(0.1 + 0.9 * jax.random.uniform(seeds[2], (TOKENS, TOPK), jnp.float32) ** steps_of(seeds[2], (TOKENS, TOPK), ((0, 16),), -0.2, 0.2), 0.1, 1.0)
    w_gate_up = bell_draw(seeds[3], (N_EP, EXP_DEV * FF, 2, D), D ** -0.5, 0.125, ((0, 16), (1, 32)))
    w_down = heavy_noise(seeds[4], (N_EP, EXP_DEV * FF, D), FF ** -0.5, 0.3125, ((0, 16), (1, 32)), (1, 2, 32, 2.75))
    return {"tokens": tokens, "expert_ids": expert_ids, "gate_weights": gate_weights, "w_gate_up": w_gate_up, "w_down": w_down}


def slot_numbers(ids, count):
    flat = ids.reshape(-1)
    onehot = (flat[:, None] == jnp.arange(count, dtype=jnp.int32)[None, :]).astype(jnp.int32)
    before = jnp.cumsum(onehot, axis=0) - onehot
    return jnp.sum(before * onehot, axis=1).astype(jnp.int32).reshape(ids.shape)


def reference(tokens, expert_ids, gate_weights, w_gate_up, w_down):
    blocks = expert_ids.reshape(N_EP, TOK_EP, TOPK)
    slot = jax.vmap(lambda b: slot_numbers(b, EXPERTS))(blocks).reshape(TOKENS, TOPK)
    token_index = jnp.broadcast_to(jnp.arange(TOKENS, dtype=jnp.int32)[:, None], (TOKENS, TOPK))
    block_index = (token_index // TOK_EP).astype(jnp.int32)
    position = (block_index * CAP + slot).astype(jnp.int32)
    table = jnp.full((EXPERTS, N_EP * CAP), TOKENS, dtype=jnp.int32).at[expert_ids, position].set(token_index)
    padded = jnp.concatenate([tokens, jnp.zeros((1, D), jnp.bfloat16)], axis=0)
    all_up = w_gate_up.reshape(EXPERTS, FF, 2, D)
    all_down = w_down.reshape(EXPERTS, FF, D)

    def per_expert(packed):
        rows_index, weights_up, weights_down = packed
        rows = padded[rows_index]
        gate = jnp.dot(rows, weights_up[:, 0, :].T, preferred_element_type=jnp.float32)
        upper = jnp.dot(rows, weights_up[:, 1, :].T, preferred_element_type=jnp.float32)
        hidden = (jax.nn.silu(gate) * upper).astype(jnp.bfloat16)
        count = rows.shape[0]
        grouped = hidden.reshape(count, SHARDS, FF // SHARDS).astype(jnp.float32)
        down = weights_down.reshape(SHARDS, FF // SHARDS, D).astype(jnp.float32)
        parts = jnp.einsum("rjf,jfd->rjd", grouped, down)
        parts = lax.optimization_barrier(parts.astype(jnp.bfloat16)).astype(jnp.float32)
        return jnp.sum(parts, axis=1).astype(jnp.bfloat16)

    results = lax.map(per_expert, (table, all_up, all_down))
    flat = results.reshape(EXPERTS * N_EP * CAP, D)
    picked = flat[(expert_ids * (N_EP * CAP) + position).astype(jnp.int32)]
    mixed = jnp.sum(picked.astype(jnp.float32) * gate_weights[:, :, None], axis=1)
    return mixed.astype(jnp.bfloat16)
```

```python
import jax
import jax.numpy as jnp
from jax import lax
from jax.sharding import Mesh
from jax.sharding import PartitionSpec as P

EXP_DEV = 4
BF16, F32 = jnp.bfloat16, jnp.float32
CHIPS = ("yl", "xh")
EXPERT_AXES = ("yh", "xl", "z")


def other(value, axis):
    return lax.ppermute(value, axis, [(0, 1), (1, 0)])


def across(value):
    return lax.ppermute(value, CHIPS, [(i, 3 - i) for i in range(4)])


def member_values(mine, y_side, x_side, diagonal, yl, xh):
    row_own = jnp.where(xh == 0, jnp.stack([mine, x_side]), jnp.stack([x_side, mine]))
    row_far = jnp.where(xh == 0, jnp.stack([y_side, diagonal]), jnp.stack([diagonal, y_side]))
    return jnp.where(yl == 0, jnp.stack([row_own, row_far]), jnp.stack([row_far, row_own]))


def on_device(tokens, expert_ids, gate_weights, w_gate_up, w_down):
    yl, xh, co = (lax.axis_index(a) for a in ("yl", "xh", "co"))
    groups = lax.axis_size("xl") * lax.axis_size("z")
    experts = EXP_DEV * groups
    rows, width = tokens.shape
    topk = expert_ids.shape[1]
    half = rows * topk * 4 // (3 * experts) // 2
    wgu_far, wd_far = other(w_gate_up[0], "co"), other(w_down[0], "co")
    tok_far = other(tokens, "co")
    tok = jnp.where(
        co == 0,
        jnp.concatenate([tokens, tok_far], 1),
        jnp.concatenate([tok_far, tokens], 1),
    )
    place = (expert_ids % EXP_DEV) * groups + expert_ids // EXP_DEV
    chosen = place.T[:, None, :] == jnp.arange(experts, dtype=jnp.int32)[None, :, None]
    member = jnp.any(chosen, axis=0)
    gate_of = jnp.sum(jnp.where(chosen, gate_weights.T[:, None, :], 0.0), axis=0)
    token_no = jnp.arange(rows, dtype=jnp.int32)
    earlier = (token_no[:, None] < token_no[None, :]).astype(BF16)
    slot = jnp.dot(member.astype(BF16), earlier, preferred_element_type=F32)
    slot = jnp.where(member, slot.astype(jnp.int32), -1)
    wanted = co * half + jnp.arange(half, dtype=jnp.int32)
    hit = slot[:, None, :] == wanted[None, :, None]
    select = hit.astype(BF16).reshape(experts * half, rows)
    placed = jnp.dot(select, tok, preferred_element_type=F32).astype(BF16)
    placed = placed.reshape(experts, half, 2 * width)
    arrived = lax.all_to_all(placed, EXPERT_AXES, 0, 0, tiled=True)
    count = groups * half
    arrived = arrived.reshape(EXP_DEV, count, 2 * width)
    full = member_values(
        arrived, other(arrived, "yl"), other(arrived, "xh"), across(arrived), yl, xh
    )
    full = jnp.transpose(full, (3, 2, 0, 1, 4)).reshape(count, -1)
    outs = []
    for wgu, wd in ((w_gate_up[0], w_down[0]), (wgu_far, wd_far)):
        gu = jnp.einsum("rd,fgd->gfr", full, wgu, preferred_element_type=F32)
        hidden = (jax.nn.silu(gu[0]) * gu[1]).astype(BF16)
        outs.append((hidden, wd))
    hidden = jnp.concatenate([o[0] for o in outs], 0)
    wd = jnp.concatenate([o[1] for o in outs], 0)
    partial = jnp.einsum("fr,fd->rd", hidden, wd, preferred_element_type=F32).astype(BF16)
    pieces = partial.reshape(count, EXP_DEV, 2, 2, 2 * width).transpose(2, 3, 1, 0, 4)
    pick = lambda a, b: lax.dynamic_slice(
        pieces, (a, b, 0, 0, 0), (1, 1) + pieces.shape[2:]
    )[0, 0]
    total = (
        pick(yl, xh).astype(F32)
        + other(pick(1 - yl, xh), "yl").astype(F32)
        + other(pick(yl, 1 - xh), "xh").astype(F32)
        + across(pick(1 - yl, 1 - xh)).astype(F32)
    ).astype(BF16)
    back = lax.all_to_all(
        total.reshape(experts, half, 2 * width), EXPERT_AXES, 0, 0, tiled=True
    ).reshape(experts * half, 2 * width)
    gate_hi = gate_of.astype(BF16)
    gate_lo = (gate_of - gate_hi.astype(F32)).astype(BF16)
    weigh = jnp.stack(
        [jnp.where(hit, g[:, None, :], 0).reshape(experts * half, rows) for g in (gate_hi, gate_lo)]
    )
    mixed = jnp.einsum("pst,sd->td", weigh, back, preferred_element_type=F32)
    keep = jnp.where(co == 0, mixed[:, :width], mixed[:, width:])
    give = jnp.where(co == 0, mixed[:, width:], mixed[:, :width])
    return (keep + other(give, "co")).astype(BF16)


def solution(mesh):
    fine = Mesh(mesh.devices.reshape(4, 2, 2, 2, 2, 8), ("yh", "yl", "xh", "co", "xl", "z"))
    hid, ep = ("yh", "yl", "xh", "co"), ("xl", "z")
    return jax.shard_map(
        on_device,
        mesh=fine,
        in_specs=(
            P(ep, hid),
            P(ep, None),
            P(ep, None),
            P(ep, hid, None, None),
            P(ep, hid, None),
        ),
        out_specs=P(ep, hid),
        check_vma=False,
    )
```

```python
import functools

import jax
import jax.numpy as jnp
from jax import lax
from jax.experimental import pallas as pl
from jax.experimental.pallas import tpu as pltpu
from jax.sharding import Mesh
from jax.sharding import PartitionSpec as P

EXP_DEV = 4
BF16, F32 = jnp.bfloat16, jnp.float32
CHIPS = ("yl", "xh")
EXPERT_AXES = ("yh", "xl", "z")


def other(value, axis):
    return lax.ppermute(value, axis, [(0, 1), (1, 0)])


def across(value):
    return lax.ppermute(value, CHIPS, [(i, 3 - i) for i in range(4)])


def mlp_kernel(shards, place_ref, *refs):
    rows_in, refs = refs[:4], refs[4:]
    ups, downs, refs = refs[:shards], refs[shards : 2 * shards], refs[2 * shards :]
    outs, (full, acc) = refs[:4], refs[4:]
    yl, xh = place_ref[0], place_ref[1]
    quarters, _, lanes = rows_in[0].shape
    wide = 4 * lanes
    members = [2 * (yl ^ a) + (xh ^ b) for b in (0, 1) for a in (0, 1)]
    starts = [pl.multiple_of(m * lanes, lanes) for m in members]
    for q in range(quarters):
        for piece, start in zip(rows_in, starts):
            full[:, pl.ds(q * wide + start, lanes)] = piece[q]
    rows = full[...]
    nt = (((1,), (1,)), ((), ()))
    hidden = []
    for up in ups:
        gate = lax.dot_general(rows, up[0], nt, preferred_element_type=F32)
        value = lax.dot_general(rows, up[1], nt, preferred_element_type=F32)
        hidden.append((gate / (1.0 + jnp.exp(-gate)) * value).astype(BF16))
    for q in range(quarters):
        total = None
        for h, down in zip(hidden, downs):
            part = jnp.dot(h, down[:, q * wide : (q + 1) * wide], preferred_element_type=F32)
            total = part if total is None else total + part
        acc[...] = total
        for out, start in zip(outs, starts):
            out[q] = acc[:, pl.ds(start, lanes)].astype(BF16)


def mlp(place, rows_in, ups, downs):
    quarters, count, lanes = rows_in[0].shape
    width = downs[0].shape[1]
    hidden = downs[0].shape[0] * len(downs)
    whole = pl.BlockSpec(memory_space=pltpu.VMEM)
    return pl.pallas_call(
        functools.partial(mlp_kernel, len(downs)),
        out_shape=[jax.ShapeDtypeStruct(rows_in[0].shape, BF16)] * 4,
        in_specs=[pl.BlockSpec(memory_space=pltpu.SMEM)]
        + [whole] * (4 + 2 * len(downs)),
        out_specs=[whole] * 4,
        scratch_shapes=[
            pltpu.VMEM((count, width), BF16),
            pltpu.VMEM((count, 4 * lanes), F32),
        ],
        cost_estimate=pl.CostEstimate(
            flops=6 * count * width * hidden,
            bytes_accessed=6 * hidden * width + 8 * count * width,
            transcendentals=count * hidden,
        ),
        compiler_params=pltpu.CompilerParams(vmem_limit_bytes=32 << 20),
        name="expert_mlp",
    )(place, *rows_in, *ups, *downs)


def on_device(tokens, expert_ids, gate_weights, w_gate_up, w_down):
    yl, xh, co = (lax.axis_index(a) for a in ("yl", "xh", "co"))
    groups = lax.axis_size("xl") * lax.axis_size("z")
    experts = EXP_DEV * groups
    rows, width = tokens.shape
    topk = expert_ids.shape[1]
    capacity = rows * topk * 4 // (3 * experts)
    half, quarter = capacity // 2, capacity // 4
    up = jnp.transpose(w_gate_up[0], (1, 0, 2))
    down = w_down[0]
    up_x = other(up, "xh")
    down_x = other(down, "xh")
    ups = [up, other(up, "co"), up_x, other(up_x, "co")]
    downs = [down, other(down, "co"), down_x, other(down_x, "co")]
    tok_far = other(tokens, "co")
    tok = jnp.where(
        co == 0,
        jnp.concatenate([tokens, tok_far], 1),
        jnp.concatenate([tok_far, tokens], 1),
    )
    place = (expert_ids % EXP_DEV) * groups + expert_ids // EXP_DEV
    chosen = place.T[:, None, :] == jnp.arange(experts, dtype=jnp.int32)[None, :, None]
    member = jnp.any(chosen, axis=0)
    gate_of = jnp.sum(jnp.where(chosen, gate_weights.T[:, None, :], 0.0), axis=0)
    token_no = jnp.arange(rows, dtype=jnp.int32)
    earlier = (token_no[:, None] < token_no[None, :]).astype(BF16)
    slot = jnp.dot(member.astype(BF16), earlier, preferred_element_type=F32)
    slot = jnp.where(member, slot.astype(jnp.int32), -1)
    step = jnp.arange(half, dtype=jnp.int32)
    wanted = co * half + (xh ^ (step // quarter)) * quarter + step % quarter
    hit = slot[:, None, :] == wanted[None, :, None]
    select = hit.astype(BF16).reshape(experts * half, rows)
    placed = jnp.dot(select, tok, preferred_element_type=F32).astype(BF16)
    placed = placed.reshape(experts, half, 2 * width)
    arrived = lax.all_to_all(placed, EXPERT_AXES, 0, 0, tiled=True)
    count = groups * quarter
    arrived = arrived.reshape(experts, 2, quarter, 2 * width)
    keep = arrived[:, 0].reshape(EXP_DEV, count, 2 * width)
    give = arrived[:, 1].reshape(EXP_DEV, count, 2 * width)
    rows_in = [keep, other(keep, "yl"), other(give, "xh"), across(give)]
    own, to_y, to_x, to_far = mlp(jnp.stack([yl, xh]), rows_in, ups, downs)
    here = own.astype(F32) + other(to_y, "yl").astype(F32)
    there = other(to_x, "xh").astype(F32) + across(to_far).astype(F32)
    total = jnp.stack(
        [v.astype(BF16).reshape(experts, quarter, 2 * width) for v in (here, there)], 1
    )
    back = lax.all_to_all(
        total.reshape(experts, half, 2 * width), EXPERT_AXES, 0, 0, tiled=True
    ).reshape(experts * half, 2 * width)
    gate_hi = gate_of.astype(BF16)
    gate_lo = (gate_of - gate_hi.astype(F32)).astype(BF16)
    weigh = jnp.stack(
        [
            jnp.where(hit, g[:, None, :], 0).reshape(experts * half, rows)
            for g in (gate_hi, gate_lo)
        ]
    )
    mixed = jnp.einsum("pst,sd->td", weigh, back, preferred_element_type=F32)
    kept = jnp.where(co == 0, mixed[:, :width], mixed[:, width:])
    given = jnp.where(co == 0, mixed[:, width:], mixed[:, :width])
    return (kept + other(given, "co")).astype(BF16)


def solution(mesh):
    fine = Mesh(
        mesh.devices.reshape(4, 2, 2, 2, 2, 8), ("yh", "yl", "xh", "co", "xl", "z")
    )
    hid, ep = ("yh", "yl", "xh", "co"), ("xl", "z")
    return jax.shard_map(
        on_device,
        mesh=fine,
        in_specs=(
            P(ep, hid),
            P(ep, None),
            P(ep, None),
            P(ep, hid, None, None),
            P(ep, hid, None),
        ),
        out_specs=P(ep, hid),
        check_vma=False,
    )
```

```python
import functools

import jax
import jax.numpy as jnp
from jax import lax
from jax.experimental import pallas as pl
from jax.experimental.pallas import tpu as pltpu
from jax.sharding import Mesh
from jax.sharding import PartitionSpec as P


EXP_DEV = 4
BF16, F32 = jnp.bfloat16, jnp.float32
CORES = ("xh", "co")
EXPERT_AXES = ("yh", "xl", "z")


def other(value, axis):
    return lax.ppermute(value, axis, [(0, 1), (1, 0)])


def up_kernel(shards, place_ref, near_ref, far_ref, *refs):
    ups, (hidden_ref, full) = refs[:shards], refs[shards:]
    quarters, _, lanes = near_ref.shape
    near = pl.multiple_of(place_ref[0] * lanes, lanes)
    far = pl.multiple_of((1 - place_ref[0]) * lanes, lanes)
    for q in range(quarters):
        full[:, pl.ds(2 * q * lanes + near, lanes)] = near_ref[q]
        full[:, pl.ds(2 * q * lanes + far, lanes)] = far_ref[q]
    rows = full[...]
    nt = (((1,), (1,)), ((), ()))
    for j, up in enumerate(ups):
        gate = lax.dot_general(rows, up[0], nt, preferred_element_type=F32)
        value = lax.dot_general(rows, up[1], nt, preferred_element_type=F32)
        hidden_ref[j] = (gate / (1.0 + jnp.exp(-gate)) * value).astype(BF16)


def down_kernel(shards, place_ref, hidden_ref, *refs):
    downs, (near_ref, far_ref, acc) = refs[:shards], refs[shards:]
    quarters, _, lanes = near_ref.shape
    near = pl.multiple_of(place_ref[0] * lanes, lanes)
    far = pl.multiple_of((1 - place_ref[0]) * lanes, lanes)
    for q in range(quarters):
        total = None
        for j, down in enumerate(downs):
            part = jnp.dot(
                hidden_ref[j],
                down[:, 2 * q * lanes : 2 * (q + 1) * lanes],
                preferred_element_type=F32,
            )
            total = part if total is None else total + part
        acc[...] = total
        near_ref[q] = acc[:, pl.ds(near, lanes)].astype(BF16)
        far_ref[q] = acc[:, pl.ds(far, lanes)].astype(BF16)


WHOLE = pl.BlockSpec(memory_space=pltpu.VMEM)
SCALARS = pl.BlockSpec(memory_space=pltpu.SMEM)


def expert_up(place, near, far, ups):
    _, count, _ = near.shape
    units = ups[0].shape[1]
    width = ups[0].shape[2]
    return pl.pallas_call(
        functools.partial(up_kernel, len(ups)),
        out_shape=jax.ShapeDtypeStruct((len(ups), count, units), BF16),
        in_specs=[SCALARS, WHOLE, WHOLE] + [WHOLE] * len(ups),
        out_specs=WHOLE,
        scratch_shapes=[pltpu.VMEM((count, width), BF16)],
        cost_estimate=pl.CostEstimate(
            flops=4 * count * width * units * len(ups),
            bytes_accessed=4 * units * len(ups) * width + 2 * count * width,
            transcendentals=count * units * len(ups),
        ),
        compiler_params=pltpu.CompilerParams(vmem_limit_bytes=16 << 20),
        name="expert_up",
    )(place, near, far, *ups)


def expert_down(place, hidden, downs, lanes):
    shards, count, units = hidden.shape
    width = downs[0].shape[1]
    quarters = width // (2 * lanes)
    return pl.pallas_call(
        functools.partial(down_kernel, shards),
        out_shape=[jax.ShapeDtypeStruct((quarters, count, lanes), BF16)] * 2,
        in_specs=[SCALARS, WHOLE] + [WHOLE] * shards,
        out_specs=[WHOLE] * 2,
        scratch_shapes=[pltpu.VMEM((count, 2 * lanes), F32)],
        cost_estimate=pl.CostEstimate(
            flops=2 * count * width * units * shards,
            bytes_accessed=2 * units * shards * width + 2 * count * width,
            transcendentals=0,
        ),
        compiler_params=pltpu.CompilerParams(vmem_limit_bytes=16 << 20),
        name="expert_down",
    )(place, hidden, *downs)


def on_device(tokens, expert_ids, gate_weights, w_gate_up, w_down):
    yl, xh, co = (lax.axis_index(a) for a in ("yl", "xh", "co"))
    groups = lax.axis_size("xl") * lax.axis_size("z")
    experts = EXP_DEV * groups
    rows, width = tokens.shape
    topk = expert_ids.shape[1]
    share = rows * topk * 4 // (3 * experts) // 4
    up = jnp.transpose(w_gate_up[0], (1, 0, 2))
    down = w_down[0]
    up_x = other(up, "xh")
    down_x = other(down, "xh")
    up_c = other(up, "co")
    down_c = other(down, "co")
    tok = lax.all_gather(tokens, CORES, axis=1, tiled=True)
    place = (expert_ids % EXP_DEV) * groups + expert_ids // EXP_DEV
    chosen = place.T[:, None, :] == jnp.arange(experts, dtype=jnp.int32)[None, :, None]
    member = jnp.any(chosen, axis=0)
    gate_of = jnp.sum(jnp.where(chosen, gate_weights.T[:, None, :], 0.0), axis=0)
    gate_of = gate_of.astype(BF16)
    token_no = jnp.arange(rows, dtype=jnp.int32)
    earlier = (token_no[:, None] < token_no[None, :]).astype(BF16)
    slot = jnp.dot(member.astype(BF16), earlier, preferred_element_type=F32)
    slot = jnp.where(member, slot.astype(jnp.int32), -1)
    wanted = (2 * xh + co) * share + jnp.arange(share, dtype=jnp.int32)
    hit = slot[:, None, :] == wanted[None, :, None]
    select = hit.astype(BF16).reshape(experts * share, rows)
    placed = jnp.dot(select, tok, preferred_element_type=F32).astype(BF16)
    placed = placed.reshape(experts, share, 4 * width)
    arrived = lax.all_to_all(placed, EXPERT_AXES, 0, 0, tiled=True)
    count = groups * share
    near = arrived.reshape(EXP_DEV, count, 4 * width)
    far = other(near, "yl")
    up_xc = other(up_x, "co")
    spot = yl[None]
    hidden = expert_up(spot, near, far, [up, up_c, up_x, up_xc])
    down_x, hidden = lax.optimization_barrier((down_x, hidden))
    down_xc = other(down_x, "co")
    mine, to_far = expert_down(spot, hidden, [down, down_c, down_x, down_xc], 4 * width)
    total = (mine.astype(F32) + other(to_far, "yl").astype(F32)).astype(BF16)
    back = lax.all_to_all(
        total.reshape(experts, share, 4 * width), EXPERT_AXES, 0, 0, tiled=True
    ).reshape(experts * share, 4 * width)
    weigh = jnp.where(hit, gate_of[:, None, :], 0).reshape(
        experts * share, rows
    )
    mixed = jnp.einsum("st,sd->dt", weigh, back, preferred_element_type=F32).astype(BF16)
    parts = lax.all_to_all(
        mixed.reshape(4, width, rows), CORES, 0, 0, tiled=True
    )
    return jnp.sum(parts.astype(F32), axis=0).astype(BF16).T


def solution(mesh):
    fine = Mesh(
        mesh.devices.reshape(4, 2, 2, 2, 2, 8), ("yh", "yl", "xh", "co", "xl", "z")
    )
    hid, ep = ("yh", "yl", "xh", "co"), ("xl", "z")
    return jax.shard_map(
        on_device,
        mesh=fine,
        in_specs=(
            P(ep, hid),
            P(ep, None),
            P(ep, None),
            P(ep, hid, None, None),
            P(ep, hid, None),
        ),
        out_specs=P(ep, hid),
        check_vma=False,
    )
```

```python
import functools

import jax
import jax.numpy as jnp
from jax import lax
from jax.experimental import pallas as pl
from jax.experimental.pallas import tpu as pltpu
from jax.sharding import Mesh
from jax.sharding import PartitionSpec as P


EXP_DEV = 4
BF16, F32 = jnp.bfloat16, jnp.float32
CHIPS = ("yl", "xh")
EXPERT_AXES = ("yh", "xl", "z")


def other(value, axis):
    return lax.ppermute(value, axis, [(0, 1), (1, 0)])


def across(value):
    return lax.ppermute(value, CHIPS, [(i, 3 - i) for i in range(4)])


def up_kernel(shards, place_ref, near_ref, far_ref, *refs):
    ups, (hidden_ref, full, held, done) = refs[:shards], refs[shards:]
    copies = [
        pltpu.make_async_copy(up.at[pl.ds(0, 2)], held.at[j], done.at[j])
        for j, up in enumerate(ups)
    ]
    for copy in copies:
        copy.start()
    quarters, _, lanes = near_ref.shape
    near = pl.multiple_of(place_ref[0] * lanes, lanes)
    far = pl.multiple_of((1 - place_ref[0]) * lanes, lanes)
    for q in range(quarters):
        full[:, pl.ds(2 * q * lanes + near, lanes)] = near_ref[q]
        full[:, pl.ds(2 * q * lanes + far, lanes)] = far_ref[q]
    rows = full[...]
    nt = (((1,), (1,)), ((), ()))
    for j, copy in enumerate(copies):
        copy.wait()
        gate = lax.dot_general(rows, held[j, 0], nt, preferred_element_type=F32)
        value = lax.dot_general(rows, held[j, 1], nt, preferred_element_type=F32)
        hidden_ref[j] = (gate / (1.0 + jnp.exp(-gate)) * value).astype(BF16)


def down_kernel(shards, place_ref, hidden_ref, *refs):
    downs, outs, (acc, held, done) = refs[:shards], refs[shards:-3], refs[-3:]
    copies = [
        pltpu.make_async_copy(down.at[down.shape[0] - 1], held.at[j], done.at[j])
        for j, down in enumerate(downs)
    ]
    for copy in copies:
        copy.start()
    yl, xh = place_ref[0], place_ref[1]
    quarters, _, lanes = outs[0].shape
    wide = 4 * lanes
    members = [2 * (yl ^ a) + (xh ^ b) for b in (0, 1) for a in (0, 1)]
    starts = [pl.multiple_of(m * lanes, lanes) for m in members]
    for copy in copies:
        copy.wait()
    for q in range(quarters):
        total = None
        for j in range(shards):
            part = jnp.dot(
                hidden_ref[j],
                held[j, :, q * wide : (q + 1) * wide],
                preferred_element_type=F32,
            )
            total = part if total is None else total + part
        acc[...] = total
        for out, start in zip(outs, starts):
            out[q] = acc[:, pl.ds(start, lanes)].astype(BF16)


WHOLE = pl.BlockSpec(memory_space=pltpu.VMEM)
ANYWHERE = pl.BlockSpec(memory_space=pl.ANY)
SCALARS = pl.BlockSpec(memory_space=pltpu.SMEM)


def sum_kernel(own_ref, y_ref, x_ref, far_ref, out_ref):
    quarters, count, _ = own_ref.shape
    share = out_ref.shape[1] // 2
    pairs = ((own_ref, y_ref), (x_ref, far_ref))
    for q in range(quarters):
        for i, (a, b) in enumerate(pairs):
            total = (a[q].astype(F32) + b[q].astype(F32)).astype(BF16)
            for g in range(count // share):
                out_ref[q * (count // share) + g, i * share : (i + 1) * share] = total[
                    g * share : (g + 1) * share
                ]


def add_pieces(pieces, share):
    quarters, count, lanes = pieces[0].shape
    size = quarters * count * lanes
    return pl.pallas_call(
        sum_kernel,
        out_shape=jax.ShapeDtypeStruct(
            (quarters * count // share, 2 * share, lanes), BF16
        ),
        in_specs=[WHOLE] * 4,
        out_specs=WHOLE,
        cost_estimate=pl.CostEstimate(
            flops=2 * size, bytes_accessed=12 * size, transcendentals=0
        ),
        compiler_params=pltpu.CompilerParams(vmem_limit_bytes=8 << 20),
        name="add_pieces",
    )(*pieces)


def expert_up(place, near, far, ups):
    _, count, _ = near.shape
    _, units, width = ups[0].shape
    shards = len(ups)
    return pl.pallas_call(
        functools.partial(up_kernel, shards),
        out_shape=jax.ShapeDtypeStruct((shards, count, units), BF16),
        in_specs=[SCALARS, WHOLE, WHOLE] + [ANYWHERE] * shards,
        out_specs=WHOLE,
        scratch_shapes=[
            pltpu.VMEM((count, width), BF16),
            pltpu.VMEM((shards, 2, units, width), BF16),
            pltpu.SemaphoreType.DMA((shards,)),
        ],
        cost_estimate=pl.CostEstimate(
            flops=4 * count * width * units * shards,
            bytes_accessed=4 * units * shards * width + 2 * count * width,
            transcendentals=count * units * shards,
        ),
        compiler_params=pltpu.CompilerParams(vmem_limit_bytes=16 << 20),
        name="expert_up",
    )(place, near, far, *ups)


def expert_down(place, hidden, downs):
    shards, count, units = hidden.shape
    width = downs[0].shape[2]
    lanes = width // (4 * EXP_DEV)
    return pl.pallas_call(
        functools.partial(down_kernel, shards),
        out_shape=[jax.ShapeDtypeStruct((EXP_DEV, count, lanes), BF16)] * 4,
        in_specs=[SCALARS, WHOLE] + [ANYWHERE] * shards,
        out_specs=[WHOLE] * 4,
        scratch_shapes=[
            pltpu.VMEM((count, 4 * lanes), F32),
            pltpu.VMEM((shards, units, width), BF16),
            pltpu.SemaphoreType.DMA((shards,)),
        ],
        cost_estimate=pl.CostEstimate(
            flops=2 * count * width * units * shards,
            bytes_accessed=2 * units * shards * width + 2 * count * width,
            transcendentals=0,
        ),
        compiler_params=pltpu.CompilerParams(vmem_limit_bytes=16 << 20),
        name="expert_down",
    )(place, hidden, *downs)


def on_device(tokens, expert_ids, gate_weights, w_gate_up, w_down):
    yl, xh, co = (lax.axis_index(a) for a in ("yl", "xh", "co"))
    groups = lax.axis_size("xl") * lax.axis_size("z")
    experts = EXP_DEV * groups
    rows, width = tokens.shape
    topk = expert_ids.shape[1]
    capacity = rows * topk * 4 // (3 * experts)
    half, share = capacity // 2, capacity // 4
    tok_x = other(tokens, "xh")
    up = jnp.transpose(w_gate_up[0], (1, 0, 2))
    up_x = other(up, "xh")
    down_x = other(w_down, "xh")
    mine = jnp.concatenate([up, w_down])
    mine_c = other(mine, "co")
    pair = lax.all_gather(jnp.stack([tokens.T, tok_x.T]), "co")
    by_chip = jnp.where(xh == 0, pair, pair[:, ::-1])
    tok = jnp.transpose(by_chip, (1, 0, 2, 3)).reshape(4 * width, rows)
    place = (expert_ids % EXP_DEV) * groups + expert_ids // EXP_DEV
    chosen = place.T[:, None, :] == jnp.arange(experts, dtype=jnp.int32)[None, :, None]
    member = jnp.any(chosen, axis=0)
    gate_of = jnp.sum(jnp.where(chosen, gate_weights.T[:, None, :], 0.0), axis=0)
    gate_of = gate_of.astype(BF16)
    token_no = jnp.arange(rows, dtype=jnp.int32)
    earlier = (token_no[:, None] < token_no[None, :]).astype(BF16)
    slot = jnp.dot(member.astype(BF16), earlier, preferred_element_type=F32)
    slot = jnp.where(member, slot.astype(jnp.int32), -1)
    step = jnp.arange(half, dtype=jnp.int32)
    wanted = co * half + (xh ^ (step // share)) * share + step % share
    hit = slot[:, None, :] == wanted[None, :, None]
    select = hit[:, :share].astype(BF16).reshape(experts * share, rows)
    placed = jnp.einsum("st,dt->sd", select, tok, preferred_element_type=F32).astype(BF16)
    placed = placed.reshape(experts, share, 4 * width)
    arrived = lax.all_to_all(placed, EXPERT_AXES, 0, 0, tiled=True)
    count = groups * share
    near = arrived.reshape(EXP_DEV, count, 4 * width)
    far = other(near, "yl")
    up_xc = other(up_x, "co")
    spot = jnp.stack([yl, xh])
    hidden = expert_up(spot, near, far, [mine, mine_c, up_x, up_xc])
    down_x, hidden = lax.optimization_barrier((down_x, hidden))
    down_xc = other(down_x, "co")
    own, to_y, to_x, to_far = expert_down(
        spot, hidden, [mine, mine_c, down_x, down_xc]
    )
    from_far = across(to_far)
    total = add_pieces([own, other(to_y, "yl"), other(to_x, "xh"), from_far], share)
    back = lax.all_to_all(
        total, EXPERT_AXES, 0, 0, tiled=True
    ).reshape(experts * half, 2 * width)
    weigh = jnp.where(hit, gate_of[:, None, :], 0).reshape(experts * half, rows)
    mixed = jnp.einsum("st,sd->dt", weigh, back, preferred_element_type=F32)
    kept = jnp.where(co == 0, mixed[:width], mixed[width:])
    given = jnp.where(co == 0, mixed[width:], mixed[:width])
    return (kept + other(given, "co")).astype(BF16).T


def solution(mesh):
    fine = Mesh(
        mesh.devices.reshape(4, 2, 2, 2, 2, 8), ("yh", "yl", "xh", "co", "xl", "z")
    )
    hid, ep = ("yh", "yl", "xh", "co"), ("xl", "z")
    return jax.shard_map(
        on_device,
        mesh=fine,
        in_specs=(
            P(ep, hid),
            P(ep, None),
            P(ep, None),
            P(ep, hid, None, None),
            P(ep, hid, None),
        ),
        out_specs=P(ep, hid),
        check_vma=False,
    )
```

```python
import functools

import jax
import jax.numpy as jnp
from jax import lax
from jax.experimental import pallas as pl
from jax.experimental.layout import Layout, with_layout_constraint
from jax.experimental.pallas import tpu as pltpu
from jax.sharding import Mesh
from jax.sharding import PartitionSpec as P


EXP_DEV = 4
BF16, F32 = jnp.bfloat16, jnp.float32
ALL_CHIPS = ("yh", "yl", "xh", "xl", "z")
EXPERT_AXES = ("yh", "xl", "z")


def other(value, axis):
    return lax.ppermute(value, axis, [(0, 1), (1, 0)])


def as_given(value):
    return with_layout_constraint(value, Layout(major_to_minor=(0, 1, 2)))


def up_kernel(shards, place_ref, near_ref, far_ref, *refs):
    ups, (hidden_ref, full, held, sides, done) = refs[:shards], refs[shards:]
    copies = [
        pltpu.make_async_copy(up.at[pl.ds(0, 2)], held.at[j], done.at[j])
        for j, up in enumerate(ups)
    ]
    for copy in copies:
        copy.start()
    quarters, _, lanes = near_ref.shape
    near = pl.multiple_of(place_ref[0] * lanes, lanes)
    far = pl.multiple_of((1 - place_ref[0]) * lanes, lanes)
    for q in range(quarters):
        full[:, pl.ds(2 * q * lanes + near, lanes)] = near_ref[q]
        full[:, pl.ds(2 * q * lanes + far, lanes)] = far_ref[q]
    rows = full[...]
    nt = (((1,), (1,)), ((), ()))
    _, _, units, width = held.shape
    for j, copy in enumerate(copies):
        copy.wait()
        both = lax.dot_general(
            held[j].reshape(2 * units, width), rows, nt, preferred_element_type=F32
        )
        gate, value = both[:units], both[units:]
        sides[j * units : (j + 1) * units] = gate / (1.0 + jnp.exp(-gate)) * value
    hidden_ref[...] = sides[...].T.astype(BF16)


def down_kernel(shards, hidden_ref, *refs):
    downs, (out_ref, held, done) = refs[:shards], refs[shards:]
    units = downs[0].shape[1]
    copies = [
        pltpu.make_async_copy(
            down.at[down.shape[0] - 1], held.at[pl.ds(j * units, units)], done.at[j]
        )
        for j, down in enumerate(downs)
    ]
    for copy in copies:
        copy.start()
    for copy in copies:
        copy.wait()
    pieces, _, lanes = out_ref.shape
    wide = 4 * lanes
    for q in range(pieces // 4):
        total = jnp.dot(
            hidden_ref[...],
            held[:, q * wide : (q + 1) * wide],
            preferred_element_type=F32,
        ).astype(BF16)
        for i in range(4):
            out_ref[4 * q + i] = total[:, i * lanes : (i + 1) * lanes]


WHOLE = pl.BlockSpec(memory_space=pltpu.VMEM)
ANYWHERE = pl.BlockSpec(memory_space=pl.ANY)
SCALARS = pl.BlockSpec(memory_space=pltpu.SMEM)


def expert_up(place, near, far, ups):
    _, count, _ = near.shape
    _, units, width = ups[0].shape
    shards = len(ups)
    return pl.pallas_call(
        functools.partial(up_kernel, shards),
        out_shape=jax.ShapeDtypeStruct((count, shards * units), BF16),
        in_specs=[SCALARS, WHOLE, WHOLE] + [ANYWHERE] * shards,
        out_specs=WHOLE,
        scratch_shapes=[
            pltpu.VMEM((count, width), BF16),
            pltpu.VMEM((shards, 2, units, width), BF16),
            pltpu.VMEM((shards * units, count), F32),
            pltpu.SemaphoreType.DMA((shards,)),
        ],
        cost_estimate=pl.CostEstimate(
            flops=4 * count * width * units * shards,
            bytes_accessed=4 * units * shards * width + 2 * count * width,
            transcendentals=count * units * shards,
        ),
        compiler_params=pltpu.CompilerParams(vmem_limit_bytes=16 << 20),
        name="expert_up",
    )(place, near, far, *ups)


def expert_down(hidden, downs, lanes):
    shards, count = len(downs), hidden.shape[0]
    _, units, width = downs[0].shape
    return pl.pallas_call(
        functools.partial(down_kernel, shards),
        out_shape=jax.ShapeDtypeStruct((width // lanes, count, lanes), BF16),
        in_specs=[WHOLE] + [ANYWHERE] * shards,
        out_specs=WHOLE,
        scratch_shapes=[
            pltpu.VMEM((shards * units, width), BF16),
            pltpu.SemaphoreType.DMA((shards,)),
        ],
        cost_estimate=pl.CostEstimate(
            flops=2 * count * width * units * shards,
            bytes_accessed=2 * units * shards * width + 2 * count * width,
            transcendentals=0,
        ),
        compiler_params=pltpu.CompilerParams(vmem_limit_bytes=16 << 20),
        name="expert_down",
    )(hidden, *downs)


def on_device(tokens, expert_ids, gate_weights, w_gate_up, w_down):
    yl, xh, co = (lax.axis_index(a) for a in ("yl", "xh", "co"))
    groups = lax.axis_size("xl") * lax.axis_size("z")
    experts = EXP_DEV * groups
    rows, width = tokens.shape
    topk = expert_ids.shape[1]
    units = w_down.shape[1]
    capacity = rows * topk * 4 // (3 * experts)
    half, share = capacity // 2, capacity // 4
    early = units * 8 // 11
    early -= early % 16
    tok_x = other(tokens, "xh")
    raw_a = as_given(other(as_given(w_gate_up[0, :early]), "xh"))
    raw_b = as_given(other(as_given(w_gate_up[0, early:]), "xh"))
    down_x = other(w_down, "xh")
    mine = jnp.concatenate([jnp.transpose(w_gate_up[0], (1, 0, 2)), w_down])
    mine_c = other(mine, "co")
    pair = lax.all_gather(jnp.stack([tokens.T, tok_x.T]), "co")
    by_chip = jnp.where(xh == 0, pair, pair[:, ::-1])
    tok = jnp.transpose(by_chip, (1, 0, 2, 3)).reshape(4 * width, rows)
    place = (expert_ids % EXP_DEV) * groups + expert_ids // EXP_DEV
    chosen = place.T[:, None, :] == jnp.arange(experts, dtype=jnp.int32)[None, :, None]
    member = jnp.any(chosen, axis=0)
    gate_of = jnp.sum(jnp.where(chosen, gate_weights.T[:, None, :], 0.0), axis=0)
    gate_of = gate_of.astype(BF16)
    token_no = jnp.arange(rows, dtype=jnp.int32)
    earlier = (token_no[:, None] < token_no[None, :]).astype(BF16)
    slot = jnp.dot(member.astype(BF16), earlier, preferred_element_type=F32)
    slot = jnp.where(member, slot.astype(jnp.int32), -1)
    wanted = co * half + jnp.arange(half, dtype=jnp.int32).reshape(1, 2, 1, share, 1)
    spread = slot.reshape(EXP_DEV, 1, groups, 1, rows)
    hit = spread == wanted
    quarter = (co * 2 + xh) * share + jnp.arange(share, dtype=jnp.int32)
    select = slot[:, None, :] == quarter[None, :, None]
    select = select.astype(BF16).reshape(experts * share, rows)
    placed = jnp.einsum("st,dt->sd", select, tok, preferred_element_type=F32).astype(BF16)
    placed = placed.reshape(experts, share, 4 * width)
    arrived = lax.all_to_all(placed, EXPERT_AXES, 0, 0, tiled=True)
    count = groups * share
    near = arrived.reshape(EXP_DEV, count, 4 * width)
    far = other(near, "yl")
    up_x = jnp.transpose(jnp.concatenate([raw_a, raw_b]), (1, 0, 2))
    up_xc = other(up_x, "co")
    spot = yl[None]
    hidden = expert_up(spot, near, far, [mine, mine_c, up_x, up_xc])
    down_xc = other(down_x, "co")
    partial = expert_down(hidden, [mine, mine_c, down_x, down_xc], 2 * width)
    back = lax.all_to_all(
        partial.reshape(-1, share, 2 * width), ALL_CHIPS, 0, 0, tiled=True
    )
    back = back.reshape(EXP_DEV, 2, 2, groups, share, 2 * width).astype(F32)
    back = (back[:, 0] + back[:, 1]).astype(BF16)
    weigh = jnp.where(hit, gate_of.reshape(EXP_DEV, 1, groups, 1, rows), 0)
    mixed = jnp.einsum(
        "st,sd->dt",
        weigh.reshape(experts * half, rows),
        back.reshape(experts * half, 2 * width),
        preferred_element_type=F32,
    )
    kept = jnp.where(co == 0, mixed[:width], mixed[width:])
    given = jnp.where(co == 0, mixed[width:], mixed[:width])
    return (kept + other(given, "co")).astype(BF16).T


def solution(mesh):
    fine = Mesh(
        mesh.devices.reshape(4, 2, 2, 2, 2, 8), ("yh", "yl", "xh", "co", "xl", "z")
    )
    hid, ep = ("yh", "yl", "xh", "co"), ("xl", "z")
    return jax.shard_map(
        on_device,
        mesh=fine,
        in_specs=(
            P(ep, hid),
            P(ep, None),
            P(ep, None),
            P(ep, hid, None, None),
            P(ep, hid, None),
        ),
        out_specs=P(ep, hid),
        check_vma=False,
    )
```
